32 devices in a mesh: path: 8 (over z, x), tm: 4 (over y, core).
Axes of the slice: x: 2, y: 2, z: 4, core: 2. Of those that a mesh axis runs over, the one named last changes fastest.
Arguments:
- values: bfloat16 [128, 128, 8192], P('path', 'tm'), may hold values from -6 to 6
- trade_set: int32 [8192], replicated, may hold values from 0 to 1023
- lag_dates: int32 [1024], replicated, may hold values from 1 to 4
- threshold_cents: int32 [1024], replicated, may hold values from 200 to 1599
- cap_cents: int32 [1024], replicated, may hold values from 200 to 1599
Outputs:
- epe: float32 [128, 1024], P('tm')
- ene: float32 [128, 1024], P('tm')
The draws below stay inside these ranges and needn't reach their ends.
All inputs are finite; a program needn't handle non-finite values.
Results may differ from the reference program's by a relative error of at most 0.001.
Values may be sent and summed in bfloat16 or wider, within the bound.
A program may use at most 64 MiB of HBM per device.

```python
import jax
import jax.numpy as jnp
from jax import lax

TRADES = 8192
SETS = 1024
LAG_MAX = 4
PATH_DEV = 16
PATHS = 128
DATES = 128


def place_ends(array, rng, least, high):
    spot = [jax.random.randint(jax.random.fold_in(rng, axis), (), 0, length) for axis, length in enumerate(array.shape)]
    main_axis = array.shape.index(max(array.shape))
    beside = spot[:main_axis] + [(spot[main_axis] + 1) % array.shape[main_axis]] + spot[main_axis + 1:]
    return array.at[tuple(spot)].set(least).at[tuple(beside)].set(high)


def levels(key, dims, pieces, least, top_value):
    def one(axis_at, parts):
        draws = jax.random.uniform(jax.random.fold_in(jax.random.fold_in(key, 6), axis_at), (parts,), jnp.float32, least / len(pieces), top_value / len(pieces))
        return jnp.repeat(jnp.exp(draws), dims[axis_at] // parts).reshape((-1,) + (1,) * (len(dims) - axis_at - 1))

    level = one(*pieces[0])
    for cut in pieces[1:]:
        level = level * one(*cut)
    return level


def noise(rng, shape, width, reach, pieces=(), held_as=jnp.bfloat16):
    loudness = levels(rng, shape, pieces, -0.22, 0.18) if pieces else 1.0
    entries = jax.random.normal(rng, shape, jnp.float32) * width * loudness
    return jnp.minimum(jnp.maximum(entries, -reach), reach).astype(held_as)


def setup_inputs(seed: int = 0) -> dict:
    seeds = jax.random.split(jax.random.key(seed), 6)
    values = noise(seeds[0], (PATHS, DATES, TRADES), 1.0, 6.0, ((0, 8), (1, 4)))
    trade_set = place_ends(jax.random.randint(seeds[1], (TRADES,), 0, SETS), jax.random.fold_in(seeds[1], 1), 0, SETS - 1).astype(jnp.int32)
    lag_dates = place_ends(jax.random.randint(seeds[2], (SETS,), 1, LAG_MAX + 1), jax.random.fold_in(seeds[2], 1), 1, LAG_MAX).astype(jnp.int32)
    threshold_cents = place_ends(jax.random.randint(seeds[3], (SETS,), 200, 1600), jax.random.fold_in(seeds[3], 1), 200, 1599).astype(jnp.int32)
    cap_cents = place_ends(jax.random.randint(seeds[4], (SETS,), 200, 1600), jax.random.fold_in(seeds[4], 1), 200, 1599).astype(jnp.int32)
    return dict(values=values, trade_set=trade_set, lag_dates=lag_dates, threshold_cents=threshold_cents, cap_cents=cap_cents)


def membership(trade_set):
    set_ids = jnp.arange(SETS, dtype=jnp.int32)[None, :]
    return (trade_set[:, None] == set_ids).astype(jnp.bfloat16)


def reference(values, trade_set, lag_dates, threshold_cents, cap_cents):
    netting_book = membership(trade_set)
    lower_bound = -threshold_cents.astype(jnp.float32) / 100.0
    upper_bound = cap_cents.astype(jnp.float32) / 100.0
    blocks = values.reshape(PATHS // PATH_DEV, PATH_DEV, DATES, TRADES)

    def one_block(sums, path_block):
        netted = jnp.dot(path_block.reshape(-1, TRADES), netting_book,
                         preferred_element_type=jnp.float32).reshape(PATH_DEV, DATES, SETS)
        padded = jnp.pad(netted, ((0, 0), (LAG_MAX + 1, 0), (0, 0)))
        lagged = jnp.zeros((PATH_DEV, DATES + 1, SETS), jnp.float32)
        for offset in range(1, LAG_MAX + 1):
            lag_mask = (lag_dates == offset).astype(jnp.float32)
            lagged = lagged + lag_mask * padded[:, LAG_MAX - offset:LAG_MAX - offset + DATES + 1, :]
        margin_moves = lagged[:, 1:, :] - lagged[:, :-1, :]

        def advance(balance, change):
            balance = jnp.minimum(jnp.maximum(balance + change, lower_bound), upper_bound)
            return balance, balance

        _, collateral = lax.scan(advance, jnp.zeros((PATH_DEV, SETS), jnp.float32),
                                 jnp.swapaxes(margin_moves, 0, 1))
        net_gap = netted - jnp.swapaxes(collateral, 0, 1)
        epe_sum = sums[0] + jnp.sum(jnp.maximum(net_gap, 0.0), axis=0)
        ene_sum = sums[1] + jnp.sum(jnp.maximum(-net_gap, 0.0), axis=0)
        return (epe_sum, ene_sum), None

    zeros = jnp.zeros((DATES, SETS), jnp.float32)
    (epe_sum, ene_sum), _ = lax.scan(one_block, (zeros, zeros), blocks)
    return epe_sum / PATHS, ene_sum / PATHS
```

```python
import functools

import jax
import jax.numpy as jnp
from jax import lax
from jax.experimental import pallas as pl
from jax.experimental.pallas import tpu as pltpu
from jax.sharding import PartitionSpec as P

LAG_MAX = 4
RIM = LAG_MAX + 1
LANES = 128
F32 = jnp.float32
BF16 = jnp.bfloat16
MESH = pl.DeviceIdType.MESH


def clip(x, low, high):
    return jnp.minimum(jnp.maximum(x, low), high)


def kernel(
    path_count, tm_count, paths, dates, width, depth,
    values_ref, trades_ref, lags_ref, bounds_ref, out_ref,
    held, netted, outbox, inbox, sums, parts, pieces, finals,
    load_sem, tm_send, tm_recv, rs_send, rs_recv, ag_send, ag_recv,
):
    rows, trades = values_ref.shape
    sets = lags_ref.shape[1]
    chunks = sets // width
    tiles = width // LANES
    steps = trades // depth
    piece_rows = parts.shape[2]
    here_path, here_tm = lax.axis_index("path"), lax.axis_index("tm")

    def load(step):
        columns = pl.ds(pl.multiple_of(step * depth, depth), depth)
        return pltpu.make_async_copy(values_ref.at[:, columns], held.at[:, columns], load_sem.at[step])

    for step in range(steps):
        load(step).start()

    def greet(j, carry):
        pl.semaphore_signal(
            barrier, inc=1, device_id={"path": lax.rem(here_path + j, path_count)}, device_id_type=MESH
        )
        return carry

    barrier = pltpu.get_barrier_semaphore()
    lax.fori_loop(1, path_count, greet, 0)
    for j in range(1, tm_count):
        pl.semaphore_signal(
            barrier, inc=1, device_id={"tm": lax.rem(here_tm + j, tm_count)}, device_id_type=MESH
        )

    for j in range(1, tm_count):
        @pl.when(here_tm < j)
        def _(j=j):
            inbox[:, j - 1] = jnp.zeros(inbox.shape[:1] + inbox.shape[2:], BF16)

    def tm_copy(c, j):
        first, count = (2, 3 + RIM) if j == 1 else (0, 4)
        return pltpu.make_async_remote_copy(
            src_ref=outbox.at[c, pl.ds(first, count)],
            dst_ref=inbox.at[c, j - 1, pl.ds(first, count)],
            send_sem=tm_send.at[c, j - 1],
            recv_sem=tm_recv.at[c, j - 1],
            device_id={"tm": lax.rem(here_tm + j, tm_count)},
            device_id_type=MESH,
        )

    def rs_copy(c, j):
        to = lax.rem(here_path + j, path_count)
        return pltpu.make_async_remote_copy(
            src_ref=parts.at[c, to],
            dst_ref=pieces.at[c, j - 1],
            send_sem=rs_send.at[c],
            recv_sem=rs_recv.at[c],
            device_id={"path": to},
            device_id_type=MESH,
        )

    def ag_copy(c, j):
        columns = pl.ds(c * width, width)
        return pltpu.make_async_remote_copy(
            src_ref=finals.at[c],
            dst_ref=out_ref.at[here_path, :, columns],
            send_sem=ag_send.at[c],
            recv_sem=ag_recv.at[c],
            device_id={"path": lax.rem(here_path + j, path_count)},
            device_id_type=MESH,
        )

    def start_all(copy, c):
        def one(j, carry):
            copy(c, j).start()
            return carry
        lax.fori_loop(1, path_count, one, 0)

    set_rows = lax.broadcasted_iota(jnp.int32, (width, depth), 0)

    def multiply(c):
        def step_of(step, carry):
            if c == 0:
                load(step).wait()
            columns = pl.ds(pl.multiple_of(step * depth, depth), depth)
            book = jnp.where(trades_ref[:, columns] - c * width == set_rows, 1.0, 0.0).astype(BF16)
            product = lax.dot_general(
                held[:, columns], book, (((1,), (1,)), ((), ())), preferred_element_type=F32
            )
            for k in range(tiles):
                part = product[:, k * LANES:(k + 1) * LANES]
                netted[c % 2, k] = jnp.where(step == 0, part, netted[c % 2, k] + part)
            return carry
        lax.fori_loop(0, steps, step_of, 0)

    def dated(c, k, t):
        return netted[c % 2, k, pl.ds(t, paths, stride=dates), :]

    def span(c, k):
        return pl.ds(c * width + k * LANES, LANES)

    def limits(c, k):
        shape = (paths, LANES)
        low = jnp.broadcast_to(bounds_ref[0:1, span(c, k)], shape)
        high = jnp.broadcast_to(bounds_ref[1:2, span(c, k)], shape)
        return low, high

    def lag_of(c, k):
        return jnp.broadcast_to(lags_ref[0:1, span(c, k)], (paths, LANES))

    def summarize(c):
        every = range(tiles)
        bounds = [limits(c, k) for k in every]
        lags = [lag_of(c, k) for k in every]

        def advance(t, state):
            new = []
            for k in every:
                before, low_edge, high_edge = state[k]
                now = dated(c, k, t)
                move = now - before
                low, high = bounds[k]
                new.append((now, clip(low_edge + move, low, high), clip(high_edge + move, low, high)))
            return tuple(new)

        state = tuple((dated(c, k, 1), *bounds[k]) for k in every)
        state = lax.fori_loop(2, dates - RIM + 1, advance, state, unroll=True)
        cut = [s[1:] for s in state]
        for t in range(dates - RIM + 1, dates):
            state = advance(t, state)
            for k in every:
                if t < dates - 1:
                    keep = lags[k] <= dates - 1 - t
                    cut[k] = tuple(jnp.where(keep, new, old) for new, old in zip(state[k][1:], cut[k]))
        for k in every:
            lanes = pl.ds(k * LANES, LANES)
            outbox[c, 0, :, lanes] = state[k][1].astype(BF16)
            outbox[c, 1, :, lanes] = state[k][2].astype(BF16)
            outbox[c, 2, :, lanes] = dated(c, k, 0).astype(BF16)
            for back in range(RIM):
                outbox[c, 3 + back, :, lanes] = dated(c, k, dates - 1 - back).astype(BF16)
            outbox[c, 3 + RIM, :, lanes] = cut[k][0].astype(BF16)
            outbox[c, 4 + RIM, :, lanes] = cut[k][1].astype(BF16)
        for j in range(1, tm_count):
            @pl.when(here_tm + j < tm_count)
            def _(j=j):
                tm_copy(c, j).start()

    def expose(c):
        every = range(tiles)
        for j in range(1, tm_count):
            @pl.when(here_tm >= j)
            def _(j=j):
                tm_copy(c, j).wait_recv()

        def picked(masks, window):
            out = window[3]
            for index in (2, 1, 0):
                out = jnp.where(masks[index], window[index], out)
            return out

        masks, state = [], []
        for k in every:
            lanes = pl.ds(k * LANES, LANES)
            low, high = limits(c, k)
            lag = lag_of(c, k)
            mask = [lag == offset for offset in range(1, LAG_MAX)]

            def got(j, index):
                return inbox[c, j - 1, index, :, lanes].astype(F32)

            balance = jnp.zeros((paths, LANES), F32)
            last = balance
            for j in range(tm_count - 1, 1, -1):
                first, end = got(j, 2), got(j, 3)
                balance = clip(balance + (first - last), low, high)
                balance = clip(balance + (end - first), got(j, 0), got(j, 1))
                last = end
            first = got(1, 2)
            rim = [got(1, 3 + back) for back in range(RIM)]
            lagged = picked(mask, rim[1:])
            balance = clip(balance + (first - last), low, high)
            balance = jnp.where(here_tm > 0, balance, 0.0)
            balance = clip(balance + (lagged - first), got(1, 3 + RIM), got(1, 4 + RIM))
            masks.append(mask)
            state.append((balance, lagged, *rim[:LAG_MAX]))
        bounds = [limits(c, k) for k in every]

        def advance(t, state):
            new = []
            for k in every:
                balance, before, *window = state[k]
                low, high = bounds[k]
                now = dated(c, k, t)
                lagged = picked(masks[k], window)
                balance = clip(balance + (lagged - before), low, high)
                gap = now - balance
                above = jnp.maximum(gap, 0.0)
                below = above - gap
                for side, amount in enumerate((above, below)):
                    folded = amount[0:8]
                    for at in range(8, paths, 8):
                        folded = folded + amount[at:at + 8]
                    sums[k, pl.ds(pl.multiple_of((side * dates + t) * 8, 8), 8), :] = folded
                new.append((balance, lagged, now, *window[:LAG_MAX - 1]))
            return tuple(new)

        lax.fori_loop(0, dates, advance, tuple(state), unroll=True)
        for k in every:
            total = sums[k, pl.ds(0, 2 * dates, stride=8), :]
            for at in range(1, 8):
                total = total + sums[k, pl.ds(at, 2 * dates, stride=8), :]
            total = total.reshape(path_count, piece_rows, LANES)
            parts[c, :, :, pl.ds(k * LANES, LANES)] = total.astype(BF16)
        start_all(rs_copy, c)

    def arrived(ref, sem):
        return pltpu.make_async_copy(ref, ref, sem)

    def finish(c):
        box = pieces.at[c]
        arrived(box, rs_recv.at[c]).wait()
        total = parts[c, here_path].astype(F32)
        for j in range(path_count - 1):
            total = total + pieces[c, j].astype(F32)
        total = total * (1.0 / (paths * path_count))
        finals[c] = total
        out_ref[here_path, :, pl.ds(c * width, width)] = total
        start_all(ag_copy, c)

    for c in range(chunks):
        multiply(c)
        if c == 0:
            pl.semaphore_wait(barrier, path_count + tm_count - 2)
        summarize(c)
        if c >= 1:
            expose(c - 1)
        if c >= 2:
            finish(c - 2)
    expose(chunks - 1)
    for c in range(max(0, chunks - 2), chunks):
        finish(c)
    for c in range(chunks):
        for j in range(1, tm_count):
            @pl.when(here_tm + j < tm_count)
            def _(j=j):
                tm_copy(c, j).wait_send()
        arrived(pieces.at[c], rs_send.at[c]).wait()
        box = out_ref.at[pl.ds(0, path_count - 1), :, pl.ds(c * width, width)]
        arrived(box, ag_send.at[c]).wait()
        arrived(box, ag_recv.at[c]).wait()


def solution(mesh):
    path_count, tm_count = mesh.shape["path"], mesh.shape["tm"]

    def local(values, trade_set, lag_dates, threshold_cents, cap_cents):
        paths, dates, trades = values.shape
        sets = lag_dates.shape[0]
        width = 2 * LANES
        depth = 1024
        chunks, steps, tiles = sets // width, trades // depth, width // LANES
        piece_rows = 2 * dates // path_count
        rows = paths * dates
        bounds = jnp.stack(
            [-threshold_cents.astype(F32) / 100.0, cap_cents.astype(F32) / 100.0]
        )
        dma = pltpu.SemaphoreType.DMA
        out = pl.pallas_call(
            functools.partial(kernel, path_count, tm_count, paths, dates, width, depth),
            out_shape=jax.ShapeDtypeStruct((path_count, piece_rows, sets), F32),
            in_specs=[pl.BlockSpec(memory_space=pl.ANY)] + [pl.BlockSpec(memory_space=pltpu.VMEM)] * 3,
            out_specs=pl.BlockSpec(memory_space=pltpu.VMEM),
            scratch_shapes=[
                pltpu.VMEM((rows, trades), BF16),
                pltpu.VMEM((2, tiles, rows, LANES), F32),
                pltpu.VMEM((chunks, 5 + RIM, paths, width), BF16),
                pltpu.VMEM((chunks, tm_count - 1, 5 + RIM, paths, width), BF16),
                pltpu.VMEM((tiles, 2 * dates * 8, LANES), F32),
                pltpu.VMEM((chunks, path_count, piece_rows, width), BF16),
                pltpu.VMEM((chunks, path_count - 1, piece_rows, width), BF16),
                pltpu.VMEM((chunks, piece_rows, width), F32),
                dma((steps,)),
                dma((chunks, tm_count - 1)),
                dma((chunks, tm_count - 1)),
                dma((chunks,)),
                dma((chunks,)),
                dma((chunks,)),
                dma((chunks,)),
            ],
            compiler_params=pltpu.CompilerParams(
                collective_id=0, has_side_effects=True, vmem_limit_bytes=48 * 2**20
            ),
        )(values.reshape(rows, trades), trade_set[None, :], lag_dates[None, :], bounds)
        out = out.reshape(2 * dates, sets)
        return out[:dates], out[dates:]

    placed = (P("path", "tm", None), P(), P(), P(), P())
    return jax.shard_map(
        local, mesh=mesh, in_specs=placed, out_specs=(P("tm", None), P("tm", None)), check_vma=False
    )
```

```python
import functools

import jax
import jax.numpy as jnp
from jax import lax
from jax.experimental import pallas as pl
from jax.experimental.pallas import tpu as pltpu
from jax.sharding import PartitionSpec as P

LAG_MAX = 4
RIM = LAG_MAX + 1
LANES = 128
GROUP = 2 * LANES
F32 = jnp.float32
BF16 = jnp.bfloat16
MESH = pl.DeviceIdType.MESH


def clip(x, low, high):
    return jnp.minimum(jnp.maximum(x, low), high)


def kernel(
    path_count, tm_count, paths, dates, blocks, depths, owners,
    values_ref, trades_hbm, lags_hbm, thresholds_hbm, caps_hbm, out_ref,
    held, trades_ref, lags_ref, thresholds_ref, caps_ref,
    netted, outbox, inbox, sums, parts, pieces, finals,
    load_sem, small_sem, tm_send, tm_recv, rs_send, rs_recv, ag_send, ag_recv,
):
    rows, trades = values_ref.shape
    tiles = GROUP // LANES
    groups = lags_ref.shape[1] // GROUP
    depth = depths[0]
    piece_rows = parts.shape[1]
    base = (path_count - owners) // 2
    here_path, here_tm = lax.axis_index("path"), lax.axis_index("tm")
    place = here_path - base
    owns = jnp.logical_and(place >= 0, place < owners)

    small = [
        pltpu.make_async_copy(src, dst, small_sem.at[at])
        for at, (src, dst) in enumerate(
            ((trades_hbm, trades_ref), (lags_hbm, lags_ref), (thresholds_hbm, thresholds_ref), (caps_hbm, caps_ref))
        )
    ]

    def load(step):
        columns = pl.ds(pl.multiple_of(step * depth, depth), depth)
        return pltpu.make_async_copy(values_ref.at[:, columns], held.at[:, columns], load_sem.at[step])

    small[0].start()
    for step in range(trades // depth):
        load(step).start()
    for copy in small[1:]:
        copy.start()

    def greet(j, carry):
        pl.semaphore_signal(
            barrier, inc=1, device_id={"path": lax.rem(here_path + j, path_count)}, device_id_type=MESH
        )
        return carry

    barrier = pltpu.get_barrier_semaphore()
    lax.fori_loop(1, path_count, greet, 0)
    for j in range(1, tm_count):
        pl.semaphore_signal(
            barrier, inc=1, device_id={"tm": lax.rem(here_tm + j, tm_count)}, device_id_type=MESH
        )

    for j in range(1, tm_count):
        @pl.when(here_tm < j)
        def _(j=j):
            inbox[j - 1] = jnp.zeros(inbox.shape[1:], BF16)

    def lanes_of(g):
        return pl.ds(g * GROUP, GROUP)

    def tm_copy(g, j):
        first, count = (2, 3 + RIM) if j == 1 else (0, 4)
        return pltpu.make_async_remote_copy(
            src_ref=outbox.at[pl.ds(first, count), :, lanes_of(g)],
            dst_ref=inbox.at[j - 1, pl.ds(first, count), :, lanes_of(g)],
            send_sem=tm_send.at[g, j - 1],
            recv_sem=tm_recv.at[g, j - 1],
            device_id={"tm": lax.rem(here_tm + j, tm_count)},
            device_id_type=MESH,
        )

    def rs_start(g):
        def one(at, carry):
            to = base + at
            j = lax.rem(to - here_path + path_count, path_count)

            @pl.when(j > 0)
            def _():
                pltpu.make_async_remote_copy(
                    src_ref=parts.at[at, :, lanes_of(g)],
                    dst_ref=pieces.at[j - 1, :, lanes_of(g)],
                    send_sem=rs_send.at[g],
                    recv_sem=rs_recv.at[g],
                    device_id={"path": to},
                    device_id_type=MESH,
                ).start()
            return carry
        lax.fori_loop(0, owners, one, 0)

    def ag_start(g):
        def one(j, carry):
            pltpu.make_async_remote_copy(
                src_ref=finals.at[:, lanes_of(g)],
                dst_ref=out_ref.at[place, :, lanes_of(g)],
                send_sem=ag_send.at[g],
                recv_sem=ag_recv.at[g],
                device_id={"path": lax.rem(here_path + j, path_count)},
                device_id_type=MESH,
            ).start()
            return carry
        lax.fori_loop(1, path_count, one, 0)

    def multiply(b):
        begin, width = blocks[b]
        deep = depths[min(b, 1)]
        set_rows = lax.broadcasted_iota(jnp.int32, (width, deep), 0) + begin

        def step_of(step, carry):
            if b == 0:
                load(step).wait()
            columns = pl.ds(pl.multiple_of(step * deep, deep), deep)
            book = jnp.where(trades_ref[:, columns] == set_rows, 1.0, 0.0).astype(BF16)
            product = lax.dot_general(
                held[:, columns], book, (((1,), (1,)), ((), ())), preferred_element_type=F32
            )
            for k in range(width // LANES):
                part = product[:, k * LANES:(k + 1) * LANES]
                if trades // deep == 1:
                    netted[b % 2, k] = part
                else:
                    netted[b % 2, k] = jnp.where(step == 0, part, netted[b % 2, k] + part)
            return carry

        if trades // deep == 1:
            step_of(0, 0)
        else:
            lax.fori_loop(0, trades // deep, step_of, 0)

    def block_of(g):
        return next(b for b, (begin, width) in enumerate(blocks) if begin <= g * GROUP < begin + width)

    def dated(g, k, t):
        b = block_of(g)
        tile = (g * GROUP - blocks[b][0]) // LANES + k
        return netted[b % 2, tile, pl.ds(t, paths, stride=dates), :]

    def span(g, k):
        return pl.ds(g * GROUP + k * LANES, LANES)

    def limits(c, k):
        shape = (paths, LANES)
        low = jnp.broadcast_to(-thresholds_ref[:, span(c, k)].astype(F32) / 100.0, shape)
        high = jnp.broadcast_to(caps_ref[:, span(c, k)].astype(F32) / 100.0, shape)
        return low, high

    def lag_of(c, k):
        return jnp.broadcast_to(lags_ref[0:1, span(c, k)], (paths, LANES))

    def summarize(c):
        every = range(tiles)
        bounds = [limits(c, k) for k in every]
        lags = [lag_of(c, k) for k in every]

        def advance(t, state):
            new = []
            for k in every:
                before, low_edge, high_edge = state[k]
                now = dated(c, k, t)
                move = now - before
                low, high = bounds[k]
                new.append((now, clip(low_edge + move, low, high), clip(high_edge + move, low, high)))
            return tuple(new)

        state = tuple((dated(c, k, 1), *bounds[k]) for k in every)
        state = lax.fori_loop(2, dates - RIM + 1, advance, state, unroll=True)
        cut = [s[1:] for s in state]
        for t in range(dates - RIM + 1, dates):
            state = advance(t, state)
            for k in every:
                if t < dates - 1:
                    keep = lags[k] <= dates - 1 - t
                    cut[k] = tuple(jnp.where(keep, new, old) for new, old in zip(state[k][1:], cut[k]))
        for k in every:
            lanes = span(c, k)
            outbox[0, :, lanes] = state[k][1].astype(BF16)
            outbox[1, :, lanes] = state[k][2].astype(BF16)
            outbox[2, :, lanes] = dated(c, k, 0).astype(BF16)
            for back in range(RIM):
                outbox[3 + back, :, lanes] = dated(c, k, dates - 1 - back).astype(BF16)
            outbox[3 + RIM, :, lanes] = cut[k][0].astype(BF16)
            outbox[4 + RIM, :, lanes] = cut[k][1].astype(BF16)
        for j in range(1, tm_count):
            @pl.when(here_tm + j < tm_count)
            def _(j=j):
                tm_copy(c, j).start()

    def expose(c):
        every = range(tiles)
        for j in range(1, tm_count):
            @pl.when(here_tm >= j)
            def _(j=j):
                tm_copy(c, j).wait_recv()

        def picked(masks, window):
            out = window[3]
            for index in (2, 1, 0):
                out = jnp.where(masks[index], window[index], out)
            return out

        masks, state = [], []
        for k in every:
            lanes = span(c, k)
            low, high = limits(c, k)
            lag = lag_of(c, k)
            mask = [lag == offset for offset in range(1, LAG_MAX)]

            def got(j, index):
                return inbox[j - 1, index, :, lanes].astype(F32)

            balance = jnp.zeros((paths, LANES), F32)
            last = balance
            for j in range(tm_count - 1, 1, -1):
                first, end = got(j, 2), got(j, 3)
                balance = clip(balance + (first - last), low, high)
                balance = clip(balance + (end - first), got(j, 0), got(j, 1))
                last = end
            first = got(1, 2)
            rim = [got(1, 3 + back) for back in range(RIM)]
            lagged = picked(mask, rim[1:])
            balance = clip(balance + (first - last), low, high)
            balance = jnp.where(here_tm > 0, balance, 0.0)
            balance = clip(balance + (lagged - first), got(1, 3 + RIM), got(1, 4 + RIM))
            masks.append(mask)
            state.append((balance, lagged, *rim[:LAG_MAX]))
        bounds = [limits(c, k) for k in every]

        def advance(t, state):
            new = []
            for k in every:
                balance, before, *window = state[k]
                low, high = bounds[k]
                now = dated(c, k, t)
                lagged = picked(masks[k], window)
                balance = clip(balance + (lagged - before), low, high)
                gap = now - balance
                above = jnp.maximum(gap, 0.0)
                below = above - gap
                for side, amount in enumerate((above, below)):
                    folded = amount[0:8]
                    for at in range(8, paths, 8):
                        folded = folded + amount[at:at + 8]
                    sums[k, pl.ds(pl.multiple_of((side * dates + t) * 8, 8), 8), :] = folded
                new.append((balance, lagged, now, *window[:LAG_MAX - 1]))
            return tuple(new)

        lax.fori_loop(0, dates, advance, tuple(state), unroll=True)
        for k in every:
            total = sums[k, pl.ds(0, 2 * dates, stride=8), :]
            for at in range(1, 8):
                total = total + sums[k, pl.ds(at, 2 * dates, stride=8), :]
            parts[:, :, span(c, k)] = total.reshape(owners, piece_rows, LANES).astype(BF16)
        rs_start(c)

    def arrived(ref, sem):
        return pltpu.make_async_copy(ref, ref, sem)

    def finish(g):
        lanes = lanes_of(g)

        @pl.when(owns)
        def _():
            arrived(pieces.at[:, :, lanes], rs_recv.at[g]).wait()
            total = parts[place, :, lanes].astype(F32)
            for j in range(path_count - 1):
                total = total + pieces[j, :, lanes].astype(F32)
            total = total * (1.0 / (paths * path_count))
            finals[:, lanes] = total
            out_ref[place, :, lanes] = total
            ag_start(g)

    summarized, exposed, finished = [], [], []
    for b, (begin, width) in enumerate(blocks):
        if b == 0:
            small[0].wait()
        multiply(b)
        if b == 0:
            for copy in small[1:]:
                copy.wait()
            pl.semaphore_wait(barrier, path_count + tm_count - 2)
        fresh = list(range(begin // GROUP, (begin + width) // GROUP))
        for g in fresh:
            summarize(g)
        ready = [g for g in summarized if g not in exposed]
        due = [g for g in exposed if g not in finished]
        summarized += fresh
        for g in ready:
            expose(g)
            exposed.append(g)
        for g in due:
            finish(g)
            finished.append(g)
    for g in range(groups):
        if g not in exposed:
            expose(g)
    for g in range(groups):
        if g not in finished:
            finish(g)
    for g in range(groups):
        lanes = lanes_of(g)
        for j in range(1, tm_count):
            @pl.when(here_tm + j < tm_count)
            def _(j=j):
                tm_copy(g, j).wait_send()

        @pl.when(owns)
        def _():
            arrived(pieces.at[:, :, lanes].at[pl.ds(0, owners - 1)], rs_send.at[g]).wait()
            arrived(out_ref.at[pl.ds(0, owners - 1), :, lanes], ag_recv.at[g]).wait()
            arrived(pieces.at[:, :, pl.ds(0, 2 * GROUP)], ag_send.at[g]).wait()

        @pl.when(jnp.logical_not(owns))
        def _():
            arrived(parts.at[:, :, lanes], rs_send.at[g]).wait()
            arrived(out_ref.at[:, :, lanes], ag_recv.at[g]).wait()


def solution(mesh):
    path_count, tm_count = mesh.shape["path"], mesh.shape["tm"]

    def local(values, trade_set, lag_dates, threshold_cents, cap_cents):
        paths, dates, trades = values.shape
        sets = lag_dates.shape[0]
        owners = max(1, path_count // 2)
        piece_rows = 2 * dates // owners
        rows, groups, tiles = paths * dates, sets // GROUP, GROUP // LANES
        head = max(1, groups // 2) * GROUP
        blocks = [(0, head)] + [(at, GROUP) for at in range(head, sets, GROUP)]
        depths = (trades // 4, trades // 2)
        dma = pltpu.SemaphoreType.DMA
        out = pl.pallas_call(
            functools.partial(kernel, path_count, tm_count, paths, dates, blocks, depths, owners),
            out_shape=jax.ShapeDtypeStruct((owners, piece_rows, sets), F32),
            in_specs=[pl.BlockSpec(memory_space=pltpu.HBM)] * 5,
            out_specs=pl.BlockSpec(memory_space=pltpu.VMEM),
            scratch_shapes=[
                pltpu.VMEM((rows, trades), BF16),
                pltpu.VMEM((1, trades), jnp.int32),
                pltpu.VMEM((1, sets), jnp.int32),
                pltpu.VMEM((1, sets), jnp.int32),
                pltpu.VMEM((1, sets), jnp.int32),
                pltpu.VMEM((2, head // LANES, rows, LANES), F32),
                pltpu.VMEM((5 + RIM, paths, sets), BF16),
                pltpu.VMEM((tm_count - 1, 5 + RIM, paths, sets), BF16),
                pltpu.VMEM((tiles, 2 * dates * 8, LANES), F32),
                pltpu.VMEM((owners, piece_rows, sets), BF16),
                pltpu.VMEM((path_count - 1, piece_rows, sets), BF16),
                pltpu.VMEM((piece_rows, sets), F32),
                dma((trades // depths[0],)),
                dma((4,)),
                dma((groups, tm_count - 1)),
                dma((groups, tm_count - 1)),
                dma((groups,)),
                dma((groups,)),
                dma((groups,)),
                dma((groups,)),
            ],
            compiler_params=pltpu.CompilerParams(
                collective_id=0, has_side_effects=True, vmem_limit_bytes=56 * 2**20
            ),
        )(
            values.reshape(rows, trades), trade_set[None, :], lag_dates[None, :],
            threshold_cents[None, :], cap_cents[None, :],
        )
        out = out.reshape(2 * dates, sets)
        return out[:dates], out[dates:]

    placed = (P("path", "tm", None), P(), P(), P(), P())
    return jax.shard_map(
        local, mesh=mesh, in_specs=placed, out_specs=(P("tm", None), P("tm", None)), check_vma=False
    )
```

```python
import functools

import jax
import jax.numpy as jnp
from jax import lax
from jax.experimental import pallas as pl
from jax.experimental.pallas import tpu as pltpu
from jax.sharding import PartitionSpec as P

LAG_MAX = 4
RIM = LAG_MAX + 1
LANES = 128
GROUP = 2 * LANES
F32 = jnp.float32
BF16 = jnp.bfloat16
MESH = pl.DeviceIdType.MESH


def clip(x, low, high):
    return jnp.minimum(jnp.maximum(x, low), high)


def kernel(
    path_count, tm_count, paths, dates, blocks, depths, owners,
    values_ref, trades_hbm, lags_hbm, thresholds_hbm, caps_hbm, out_ref,
    held, trades_ref, lags_ref, thresholds_ref, caps_ref,
    netted, outbox, inbox, sums, parts, pieces, finals,
    load_sem, small_sem, tm_send, tm_recv, rs_send, rs_recv, ag_send, ag_recv,
):
    rows, trades = values_ref.shape
    tiles = GROUP // LANES
    groups = lags_ref.shape[1] // GROUP
    depth = depths[0]
    piece_rows = parts.shape[1]
    base = (path_count - owners) // 2
    here_path, here_tm = lax.axis_index("path"), lax.axis_index("tm")
    place = here_path - base
    owns = jnp.logical_and(place >= 0, place < owners)

    small = [
        pltpu.make_async_copy(src, dst, small_sem.at[at])
        for at, (src, dst) in enumerate(
            ((trades_hbm, trades_ref), (lags_hbm, lags_ref), (thresholds_hbm, thresholds_ref), (caps_hbm, caps_ref))
        )
    ]

    def load(step):
        columns = pl.ds(pl.multiple_of(step * depth, depth), depth)
        return pltpu.make_async_copy(values_ref.at[:, columns], held.at[:, columns], load_sem.at[step])

    small[0].start()
    for step in range(trades // depth):
        load(step).start()
    for copy in small[1:]:
        copy.start()

    def greet(j, carry):
        pl.semaphore_signal(
            barrier, inc=1, device_id={"path": lax.rem(here_path + j, path_count)}, device_id_type=MESH
        )
        return carry

    barrier = pltpu.get_barrier_semaphore()
    lax.fori_loop(1, path_count, greet, 0)
    for j in range(1, tm_count):
        pl.semaphore_signal(
            barrier, inc=1, device_id={"tm": lax.rem(here_tm + j, tm_count)}, device_id_type=MESH
        )

    for j in range(1, tm_count):
        @pl.when(here_tm < j)
        def _(j=j):
            inbox[j - 1] = jnp.zeros(inbox.shape[1:], BF16)

    def lanes_of(g):
        return pl.ds(g * GROUP, GROUP)

    def tm_copy(g, j):
        first, count = (2, 3 + RIM) if j == 1 else (0, 4)
        return pltpu.make_async_remote_copy(
            src_ref=outbox.at[pl.ds(first, count), :, lanes_of(g)],
            dst_ref=inbox.at[j - 1, pl.ds(first, count), :, lanes_of(g)],
            send_sem=tm_send.at[g, j - 1],
            recv_sem=tm_recv.at[g, j - 1],
            device_id={"tm": lax.rem(here_tm + j, tm_count)},
            device_id_type=MESH,
        )

    def rs_start(g):
        def one(at, carry):
            to = base + at
            j = lax.rem(to - here_path + path_count, path_count)

            @pl.when(j > 0)
            def _():
                pltpu.make_async_remote_copy(
                    src_ref=parts.at[at, :, lanes_of(g)],
                    dst_ref=pieces.at[j - 1, :, lanes_of(g)],
                    send_sem=rs_send.at[g],
                    recv_sem=rs_recv.at[g],
                    device_id={"path": to},
                    device_id_type=MESH,
                ).start()
            return carry
        lax.fori_loop(0, owners, one, 0)

    def ag_start(g):
        def one(j, carry):
            pltpu.make_async_remote_copy(
                src_ref=finals.at[:, lanes_of(g)],
                dst_ref=out_ref.at[place, :, lanes_of(g)],
                send_sem=ag_send.at[g],
                recv_sem=ag_recv.at[g],
                device_id={"path": lax.rem(here_path + j, path_count)},
                device_id_type=MESH,
            ).start()
            return carry
        lax.fori_loop(1, path_count, one, 0)

    def multiply(b):
        begin, width = blocks[b]
        deep = depths[min(b, 1)]
        set_rows = lax.broadcasted_iota(jnp.int32, (width, deep), 0) + begin

        def step_of(step, carry):
            if b == 0:
                load(step).wait()
            columns = pl.ds(pl.multiple_of(step * deep, deep), deep)
            book = jnp.where(trades_ref[:, columns] == set_rows, 1.0, 0.0).astype(BF16)
            product = lax.dot_general(
                held[:, columns], book, (((1,), (1,)), ((), ())), preferred_element_type=F32
            )
            for k in range(width // LANES):
                part = product[:, k * LANES:(k + 1) * LANES]
                if trades // deep == 1:
                    netted[b % 2, k] = part
                else:
                    netted[b % 2, k] = jnp.where(step == 0, part, netted[b % 2, k] + part)
            return carry

        if trades // deep == 1:
            step_of(0, 0)
        else:
            lax.fori_loop(0, trades // deep, step_of, 0)

    def block_of(g):
        return next(b for b, (begin, width) in enumerate(blocks) if begin <= g * GROUP < begin + width)

    def dated(g, k, t):
        b = block_of(g)
        tile = (g * GROUP - blocks[b][0]) // LANES + k
        return netted[b % 2, tile, pl.ds(t, paths, stride=dates), :]

    def span(g, k):
        return pl.ds(g * GROUP + k * LANES, LANES)

    def limits(c, k):
        shape = (paths, LANES)
        low = jnp.broadcast_to(-thresholds_ref[:, span(c, k)].astype(F32) / 100.0, shape)
        high = jnp.broadcast_to(caps_ref[:, span(c, k)].astype(F32) / 100.0, shape)
        return low, high

    def lag_of(c, k):
        return jnp.broadcast_to(lags_ref[0:1, span(c, k)], (paths, LANES))

    def summarize(c):
        every = range(tiles)
        bounds = [limits(c, k) for k in every]
        lags = [lag_of(c, k) for k in every]

        def advance(t, state):
            new = []
            for k in every:
                before, low_edge, high_edge = state[k]
                now = dated(c, k, t)
                move = now - before
                low, high = bounds[k]
                new.append((now, clip(low_edge + move, low, high), clip(high_edge + move, low, high)))
            return tuple(new)

        state = tuple((dated(c, k, 1), *bounds[k]) for k in every)
        state = lax.fori_loop(2, dates - RIM + 1, advance, state, unroll=True)
        cut = [s[1:] for s in state]
        for t in range(dates - RIM + 1, dates):
            state = advance(t, state)
            for k in every:
                if t < dates - 1:
                    keep = lags[k] <= dates - 1 - t
                    cut[k] = tuple(jnp.where(keep, new, old) for new, old in zip(state[k][1:], cut[k]))
        for k in every:
            lanes = span(c, k)
            outbox[0, :, lanes] = state[k][1].astype(BF16)
            outbox[1, :, lanes] = state[k][2].astype(BF16)
            outbox[2, :, lanes] = dated(c, k, 0).astype(BF16)
            for back in range(RIM):
                outbox[3 + back, :, lanes] = dated(c, k, dates - 1 - back).astype(BF16)
            outbox[3 + RIM, :, lanes] = cut[k][0].astype(BF16)
            outbox[4 + RIM, :, lanes] = cut[k][1].astype(BF16)
        for j in range(1, tm_count):
            @pl.when(here_tm + j < tm_count)
            def _(j=j):
                tm_copy(c, j).start()

    def expose(c):
        every = range(tiles)
        for j in range(1, tm_count):
            @pl.when(here_tm >= j)
            def _(j=j):
                tm_copy(c, j).wait_recv()

        def picked(masks, window):
            out = window[3]
            for index in (2, 1, 0):
                out = jnp.where(masks[index], window[index], out)
            return out

        masks, state = [], []
        for k in every:
            lanes = span(c, k)
            low, high = limits(c, k)
            lag = lag_of(c, k)
            mask = [lag == offset for offset in range(1, LAG_MAX)]

            def got(j, index):
                return inbox[j - 1, index, :, lanes].astype(F32)

            balance = jnp.zeros((paths, LANES), F32)
            last = balance
            for j in range(tm_count - 1, 1, -1):
                first, end = got(j, 2), got(j, 3)
                balance = clip(balance + (first - last), low, high)
                balance = clip(balance + (end - first), got(j, 0), got(j, 1))
                last = end
            first = got(1, 2)
            rim = [got(1, 3 + back) for back in range(RIM)]
            lagged = picked(mask, rim[1:])
            balance = clip(balance + (first - last), low, high)
            balance = jnp.where(here_tm > 0, balance, 0.0)
            balance = clip(balance + (lagged - first), got(1, 3 + RIM), got(1, 4 + RIM))
            masks.append(mask)
            state.append((balance, lagged, *rim[:LAG_MAX]))
        bounds = [limits(c, k) for k in every]

        def advance(t, state):
            new = []
            for k in every:
                balance, before, *window = state[k]
                low, high = bounds[k]
                now = dated(c, k, t)
                lagged = picked(masks[k], window)
                balance = clip(balance + (lagged - before), low, high)
                gap = now - balance
                above = jnp.maximum(gap, 0.0)
                below = above - gap
                for side, amount in enumerate((above, below)):
                    folded = amount[0:8]
                    for at in range(8, paths, 8):
                        folded = folded + amount[at:at + 8]
                    sums[k, pl.ds(pl.multiple_of((side * dates + t) * 8, 8), 8), :] = folded
                new.append((balance, lagged, now, *window[:LAG_MAX - 1]))
            return tuple(new)

        lax.fori_loop(0, dates, advance, tuple(state), unroll=True)
        for k in every:
            total = sums[k, pl.ds(0, 2 * dates, stride=8), :]
            for at in range(1, 8):
                total = total + sums[k, pl.ds(at, 2 * dates, stride=8), :]
            parts[:, :, span(c, k)] = total.reshape(owners, piece_rows, LANES)
        rs_start(c)

    def arrived(ref, sem):
        return pltpu.make_async_copy(ref, ref, sem)

    def finish(g):
        lanes = lanes_of(g)

        @pl.when(owns)
        def _():
            arrived(pieces.at[:, :, lanes], rs_recv.at[g]).wait()
            total = parts[place, :, lanes]
            for j in range(path_count - 1):
                total = total + pieces[j, :, lanes]
            total = total * (1.0 / (paths * path_count))
            finals[:, lanes] = total
            out_ref[place, :, lanes] = total
            ag_start(g)

    summarized, exposed, finished = [], [], []
    for b, (begin, width) in enumerate(blocks):
        if b == 0:
            small[0].wait()
        multiply(b)
        if b == 0:
            for copy in small[1:]:
                copy.wait()
            pl.semaphore_wait(barrier, path_count + tm_count - 2)
        fresh = list(range(begin // GROUP, (begin + width) // GROUP))
        for g in fresh:
            summarize(g)
        ready = [g for g in summarized if g not in exposed]
        due = [g for g in exposed if g not in finished]
        summarized += fresh
        for g in ready:
            expose(g)
            exposed.append(g)
        for g in due:
            finish(g)
            finished.append(g)
    for g in range(groups):
        if g not in exposed:
            expose(g)
    for g in range(groups):
        if g not in finished:
            finish(g)
    for g in range(groups):
        lanes = lanes_of(g)
        for j in range(1, tm_count):
            @pl.when(here_tm + j < tm_count)
            def _(j=j):
                tm_copy(g, j).wait_send()

        @pl.when(owns)
        def _():
            arrived(pieces.at[:, :, lanes].at[pl.ds(0, owners - 1)], rs_send.at[g]).wait()
            arrived(out_ref.at[pl.ds(0, owners - 1), :, lanes], ag_recv.at[g]).wait()
            arrived(pieces.at[:, :, lanes], ag_send.at[g]).wait()

        @pl.when(jnp.logical_not(owns))
        def _():
            arrived(parts.at[:, :, lanes], rs_send.at[g]).wait()
            arrived(out_ref.at[:, :, lanes], ag_recv.at[g]).wait()


def solution(mesh):
    path_count, tm_count = mesh.shape["path"], mesh.shape["tm"]

    def local(values, trade_set, lag_dates, threshold_cents, cap_cents):
        paths, dates, trades = values.shape
        sets = lag_dates.shape[0]
        owners = max(1, path_count // 2)
        piece_rows = 2 * dates // owners
        rows, groups, tiles = paths * dates, sets // GROUP, GROUP // LANES
        head = max(1, groups // 2) * GROUP
        blocks = [(0, head)] + [(at, GROUP) for at in range(head, sets, GROUP)]
        depths = (trades // 4, trades // 2)
        dma = pltpu.SemaphoreType.DMA
        out = pl.pallas_call(
            functools.partial(kernel, path_count, tm_count, paths, dates, blocks, depths, owners),
            out_shape=jax.ShapeDtypeStruct((owners, piece_rows, sets), F32),
            in_specs=[pl.BlockSpec(memory_space=pltpu.HBM)] * 5,
            out_specs=pl.BlockSpec(memory_space=pltpu.VMEM),
            scratch_shapes=[
                pltpu.VMEM((rows, trades), BF16),
                pltpu.VMEM((1, trades), jnp.int32),
                pltpu.VMEM((1, sets), jnp.int32),
                pltpu.VMEM((1, sets), jnp.int32),
                pltpu.VMEM((1, sets), jnp.int32),
                pltpu.VMEM((2, head // LANES, rows, LANES), F32),
                pltpu.VMEM((5 + RIM, paths, sets), BF16),
                pltpu.VMEM((tm_count - 1, 5 + RIM, paths, sets), BF16),
                pltpu.VMEM((tiles, 2 * dates * 8, LANES), F32),
                pltpu.VMEM((owners, piece_rows, sets), F32),
                pltpu.VMEM((path_count - 1, piece_rows, sets), F32),
                pltpu.VMEM((piece_rows, sets), F32),
                dma((trades // depths[0],)),
                dma((4,)),
                dma((groups, tm_count - 1)),
                dma((groups, tm_count - 1)),
                dma((groups,)),
                dma((groups,)),
                dma((groups,)),
                dma((groups,)),
            ],
            compiler_params=pltpu.CompilerParams(
                collective_id=0, has_side_effects=True, vmem_limit_bytes=56 * 2**20
            ),
        )(
            values.reshape(rows, trades), trade_set[None, :], lag_dates[None, :],
            threshold_cents[None, :], cap_cents[None, :],
        )
        out = out.reshape(2 * dates, sets)
        return out[:dates], out[dates:]

    placed = (P("path", "tm", None), P(), P(), P(), P())
    return jax.shard_map(
        local, mesh=mesh, in_specs=placed, out_specs=(P("tm", None), P("tm", None)), check_vma=False
    )
```
